32 devices in a mesh: grp: 2 (over y), row: 8 (over z, x), col: 1, ch: 2 (over core).
Axes of the slice: x: 2, y: 2, z: 4, core: 2. Of those that a mesh axis runs over, the one named last changes fastest.
Arguments:
- pair_act: bfloat16 [128, 256, 128], P('ch', ('grp', 'row'), 'col'), parts along dimension 1, may hold values from -48 to 48
- in_gain: float32 [128], P('ch'), may hold values from 0.1 to 1.9
- left_proj: bfloat16 [128, 128], P(None, 'ch'), may hold values from -0.5 to 0.5
- left_gate: bfloat16 [128, 128], P(None, 'ch'), may hold values from -0.5 to 0.5
- right_proj: bfloat16 [128, 128], P(None, 'ch'), may hold values from -0.5 to 0.5
- right_gate: bfloat16 [128, 128], P(None, 'ch'), may hold values from -0.5 to 0.5
- out_gate: bfloat16 [128, 128], P(None, 'ch'), may hold values from -0.5 to 0.5
- out_gain: float32 [128], P('ch'), may hold values from 0.1 to 1.9
- out_proj: bfloat16 [128, 128], P(None, 'ch'), may hold values from -0.5 to 0.5
Outputs:
- update: bfloat16 [128, 256, 128], P('ch', ('grp', 'row'), 'col'), parts along dimension 1
The draws below stay inside these ranges and needn't reach their ends.
There are 2 independent parts, one for each index of `grp`. The reference program is written for one: setup_inputs(seed, part) draws one part's arguments, and reference() takes and returns one part's arrays. A program takes and returns all parts, laid end to end along the dimension named above; an argument that names none is the same for every part. Nothing has to cross between parts.
All inputs are finite; a program needn't handle non-finite values.
Results may differ from the reference program's by a relative error of at most 0.0085.
Values may be sent and summed in bfloat16 or wider, within the bound.
A program may use at most 64 MiB of HBM per device.

```python
import jax
import jax.numpy as jnp
from jax import lax

C = 128
HID = 128
RES = 128


def draw_pair_act(key, part):
    keys = jax.random.split(jax.random.fold_in(key, 11), 4)
    base = jnp.clip(jax.random.normal(keys[0], (C, RES, RES), jnp.float32), -5.0, 5.0)
    channel_scale = jnp.exp(jax.random.uniform(keys[1], (C, 1, 1), jnp.float32, jnp.log(0.3), jnp.log(3.0)))
    site_scale = jnp.exp(jax.random.uniform(keys[2], (1, RES, RES), jnp.float32, jnp.log(0.3), jnp.log(3.0)))
    offset = 0.5 * jnp.clip(jax.random.normal(keys[3], (1, RES, RES), jnp.float32), -3.0, 3.0)
    return (base * channel_scale * site_scale + offset).astype(jnp.bfloat16)


def level_of(stream_key, extent, shards, low, largest):
    level = 1.0
    for position, parts in shards:
        heights = jax.random.uniform(jax.random.fold_in(jax.random.fold_in(stream_key, 6), position), (parts,), jnp.float32, low / len(shards), largest / len(shards))
        level = level * jnp.repeat(jnp.exp(heights), extent[position] // parts).reshape((-1,) + (1,) * (len(extent) - 1 - position))
    return level


def normal_values(own_key, extent, deviation, limit, shards=(), kind=jnp.bfloat16):
    entries = jax.random.normal(own_key, extent, jnp.float32) * deviation
    if len(shards) > 0:
        entries = level_of(own_key, extent, shards, -0.22, 0.18) * entries
    return jnp.clip(entries, min=-limit, max=limit).astype(kind)


def setup_inputs(seed: int = 0, part: int = 0) -> dict:
    key_list = jax.random.split(jax.random.key(seed), 10)
    part_splits = jax.random.split(jax.random.fold_in(key_list[9], part), 10)
    return {
        "pair_act": draw_pair_act(jax.random.fold_in(jax.random.fold_in(key_list[9], part), 71), part),
        "in_gain": jnp.clip(1.0 + 0.18 * jax.random.normal(key_list[1], (C,), jnp.float32), 0.1, 1.9),
        "left_proj": normal_values(key_list[2], (C, HID), C ** -0.5, 0.5, ((1, 2),)),
        "left_gate": normal_values(key_list[3], (C, HID), C ** -0.5, 0.5, ((1, 2),)),
        "right_proj": normal_values(key_list[4], (C, HID), C ** -0.5, 0.5, ((1, 2),)),
        "right_gate": normal_values(key_list[5], (C, HID), C ** -0.5, 0.5, ((1, 2),)),
        "out_gate": normal_values(key_list[6], (C, C), C ** -0.5, 0.5, ((1, 2),)),
        "out_gain": jnp.clip(1.0 + 0.18 * jax.random.normal(key_list[7], (HID,), jnp.float32), 0.1, 1.9),
        "out_proj": normal_values(key_list[8], (HID, C), HID ** -0.5, 0.5, ((1, 2),)),
    }


def layer_norm(values, gain):
    average = lax.optimization_barrier(jnp.mean(values, axis=0, keepdims=True))
    spread = lax.optimization_barrier(jnp.mean(jnp.square(values - average), axis=0, keepdims=True))
    return (values - average) * lax.rsqrt(spread + 1e-05) * gain[:, None, None]

def reference(pair_act, in_gain, left_proj, left_gate, right_proj, right_gate, out_gate, out_gain, out_proj):
    pair_float = pair_act.astype(jnp.float32)
    normed = layer_norm(pair_float, in_gain).astype(jnp.bfloat16)
    normed_float = normed.astype(jnp.float32)

    def lift_by(matrix):
        return jnp.einsum('cxy,ch->hxy', normed_float, matrix.astype(jnp.float32))
    left_edge = (jax.nn.sigmoid(lift_by(left_gate)) * lift_by(left_proj)).astype(jnp.bfloat16)
    right_edge = (jax.nn.sigmoid(lift_by(right_gate)) * lift_by(right_proj)).astype(jnp.bfloat16)
    gate_map = jax.nn.sigmoid(lift_by(out_gate))
    tri_sum = jnp.einsum('hki,hkj->hij', left_edge.astype(jnp.float32), right_edge.astype(jnp.float32))
    mid_norm = layer_norm(tri_sum, out_gain).astype(jnp.bfloat16)
    projected = jnp.einsum('hxy,hc->cxy', mid_norm.astype(jnp.float32), out_proj.astype(jnp.float32))
    return (gate_map * projected).astype(jnp.bfloat16)
```

```python
import functools

import jax
import jax.numpy as jnp
from jax import lax
from jax.experimental import pallas as pl
from jax.experimental.pallas import tpu as pltpu
from jax.sharding import PartitionSpec as P


def spread_2(value, axis, source):
    kept = jnp.where(lax.axis_index(axis) == source, value, 0).astype(value.dtype)
    return lax.psum(kept, axis)


def moments(values, channel_count):
    first_sums, squares = lax.psum(
        (jnp.sum(values, axis=0), jnp.sum(values * values, axis=0)), "ch"
    )
    average = first_sums / channel_count
    spread = squares / channel_count - average * average
    centred = values - average[None]
    return centred * lax.rsqrt(spread + 1e-05)[None]


def per_device(
    pair_act, in_gain, left_proj, left_gate, right_proj, right_gate, out_gate, out_gain, out_proj
):
    row_count = pair_act.shape[1]
    col_count = pair_act.shape[2]
    hidden = left_proj.shape[1]
    fan_out = col_count // row_count
    normed = (
        moments(pair_act.astype(jnp.float32), pair_act.shape[0] * lax.axis_size("ch"))
        * in_gain[:, None, None]
    ).astype(jnp.bfloat16)
    whole = lax.all_gather(normed, "ch", axis=0, tiled=True)
    left_weights = jnp.concatenate((left_proj, left_gate), axis=1)
    left_lifted = jnp.einsum("cxy,cn->nyx", whole, left_weights, preferred_element_type=jnp.float32)
    left_edge = (jax.nn.sigmoid(left_lifted[hidden:]) * left_lifted[:hidden]).astype(jnp.bfloat16)
    other_weights = jnp.concatenate((right_proj, right_gate, out_gate), axis=1)
    other_lifted = jnp.einsum(
        "cxy,cn->nxy", whole, other_weights, preferred_element_type=jnp.float32
    )
    right_edge = (jax.nn.sigmoid(other_lifted[hidden : 2 * hidden]) * other_lifted[:hidden]).astype(
        jnp.bfloat16
    )
    gate_map = jax.nn.sigmoid(other_lifted[2 * hidden :])
    blocks = left_edge.reshape(hidden, fan_out, row_count, row_count)
    outgoing = jnp.tile(blocks, (1, lax.axis_size("row") // fan_out, 1, 1))
    arrived = lax.all_to_all(outgoing, "row", split_axis=1, concat_axis=3, tiled=True)
    left_panel = arrived.reshape(hidden, row_count, -1)
    left_panel = spread_2(left_panel, "col", lax.axis_index("row") // fan_out)
    tri_sum = jnp.einsum(
        "hik,hkj->hij",
        left_panel,
        lax.all_gather(right_edge, "row", axis=1, tiled=True),
        preferred_element_type=jnp.float32,
    )
    mid_norm = (moments(tri_sum, hidden * lax.axis_size("ch")) * out_gain[:, None, None]).astype(
        jnp.bfloat16
    )
    all_mid = lax.all_gather(mid_norm, "ch", axis=0, tiled=True)
    projected = jnp.einsum("hxy,hc->cxy", all_mid, out_proj, preferred_element_type=jnp.float32)
    return (gate_map * projected).astype(jnp.bfloat16)


MESH = pl.DeviceIdType.MESH


def swap_major(values):
    return jnp.swapaxes(values, 0, 1)


def spread_gain(gain, lanes):
    return jnp.broadcast_to(gain, (lanes, gain.shape[1])).T


def centred_unit(values):
    count = values.shape[0]
    average = jnp.sum(values, axis=0) / count
    centred = values - average[None]
    spread = jnp.sum(centred * centred, axis=0) / count
    return centred * lax.rsqrt(spread + 1e-05)[None]


def fused_kernel(
    rows,
    act_ref,
    gain_ref,
    lp_ref,
    lg_ref,
    rp_ref,
    rg_ref,
    og_ref,
    gain2_ref,
    op_ref,
    out_ref,
    raw,
    gains,
    weights,
    normed,
    gates,
    outbox,
    inbox,
    edges,
    tri_out,
    mid,
    load_sem,
    pair_send,
    pair_recv,
    lr_send,
    lr_recv,
    tri_send,
    tri_recv,
    relay_send,
    relay_recv,
):
    me = lax.axis_index("row")
    core = lax.axis_index("ch")
    other = 1 - core
    half, depth, width = act_ref.shape
    hidden = lp_ref.shape[0]
    block = hidden // rows
    partner = {"ch": other}
    peers = [lax.rem(me + d, rows) for d in range(rows)]
    sources = [lax.rem(me + rows - d, rows) for d in range(rows)]

    loads = [pltpu.make_async_copy(act_ref, raw.at[core], load_sem.at[0])]
    for n, ref in enumerate((lp_ref, lg_ref, rp_ref, rg_ref, og_ref, op_ref)):
        loads.append(
            pltpu.make_async_copy(
                ref, weights.at[pl.ds(n * hidden, hidden)], load_sem.at[n + 1]
            )
        )
    for load in loads:
        load.start()
    barrier = pltpu.get_barrier_semaphore()
    pl.semaphore_signal(barrier, inc=1, device_id=partner, device_id_type=MESH)
    for d in range(1, rows):
        pl.semaphore_signal(barrier, inc=1, device_id={"row": peers[d]}, device_id_type=MESH)
    gains[core, 0] = spread_gain(gain_ref[...], width)
    gains[core, 1] = spread_gain(gain2_ref[...], width)
    loads[0].wait()
    pl.semaphore_wait(barrier, rows)

    def to_partner(ref, n):
        return pltpu.make_async_remote_copy(
            src_ref=ref,
            dst_ref=ref,
            send_sem=pair_send.at[n],
            recv_sem=pair_recv.at[n],
            device_id=partner,
            device_id_type=MESH,
        )

    swaps = [to_partner(raw.at[core], 0), to_partner(gains.at[core], 1)]
    for swap in swaps:
        swap.start()
    for load in loads[1:]:
        load.wait()
    for swap in swaps:
        swap.wait_recv()

    in_gain = gains[:, 0].reshape(2 * half, width)
    edge_weights = weights[pl.ds(0, 4 * hidden)]
    step = 8
    for start in range(0, depth, step):
        values = raw[:, :, pl.ds(start, step)].astype(jnp.float32)
        turned = swap_major(centred_unit(values.reshape(2 * half, step, width)))
        for x in range(step):
            operand = (turned[x] * in_gain).astype(jnp.bfloat16)
            normed[start + x] = operand
            lifted = jnp.dot(edge_weights, operand, preferred_element_type=jnp.float32)
            left = jax.nn.sigmoid(lifted[hidden : 2 * hidden]) * lifted[:hidden]
            right = jax.nn.sigmoid(lifted[3 * hidden :]) * lifted[2 * hidden : 3 * hidden]
            both = jnp.concatenate(
                (left.reshape(rows, block, width), right.reshape(rows, block, width)), axis=1
            )
            outbox[:, start + x] = both.astype(jnp.bfloat16)

    def to_peer(src, dst, d, sends, recvs):
        return pltpu.make_async_remote_copy(
            src_ref=src,
            dst_ref=dst,
            send_sem=sends.at[d],
            recv_sem=recvs.at[d],
            device_id={"row": peers[d]},
            device_id_type=MESH,
        )

    edge_copies = {
        d: to_peer(outbox.at[peers[d]], inbox.at[me], d, lr_send, lr_recv) for d in range(1, rows)
    }
    for copy in edge_copies.values():
        copy.start()

    def take_edges(box, source):
        turned = swap_major(box.astype(jnp.float32)).astype(jnp.bfloat16)
        edges[:, pl.ds(pl.multiple_of(source * depth, depth), depth)] = turned

    take_edges(outbox[me], me)
    gate_weights = weights[pl.ds(4 * hidden, hidden)]
    for x in range(depth):
        gates[x] = jax.nn.sigmoid(
            jnp.dot(gate_weights, normed[x], preferred_element_type=jnp.float32)
        )
    for d in range(1, rows):
        edge_copies[d].wait_recv()
        take_edges(inbox[sources[d]], sources[d])

    for h in range(block):
        tri_sum = lax.dot_general(
            edges[h],
            edges[block + h],
            (((0,), (0,)), ((), ())),
            preferred_element_type=jnp.float32,
        )
        tri_out[:, h] = tri_sum.astype(jnp.bfloat16).reshape(rows, depth, width)

    tri_copies = {
        d: to_peer(tri_out.at[peers[d]], mid.at[core, me], d, tri_send, tri_recv)
        for d in range(1, rows)
    }
    for copy in tri_copies.values():
        copy.start()
    mid[core, me] = tri_out[me]

    def relay(source, n, ref):
        return pltpu.make_async_remote_copy(
            src_ref=ref,
            dst_ref=mid.at[core, source],
            send_sem=relay_send.at[n],
            recv_sem=relay_recv.at[n],
            device_id=partner,
            device_id_type=MESH,
        )

    relays = [relay(me, 0, tri_out.at[me])]
    relays[0].start()
    for d in range(1, rows):
        tri_copies[d].wait_recv()
        relays.append(relay(sources[d], d, mid.at[core, sources[d]]))
        relays[d].start()
    for copy in relays:
        copy.wait_recv()

    out_gain = gains[:, 1].reshape(2 * half, width)
    out_weights = weights[pl.ds(5 * hidden, hidden)]
    for start in range(0, depth, step):
        values = mid[:, :, :, pl.ds(start, step)].astype(jnp.float32)
        turned = swap_major(centred_unit(values.reshape(2 * hidden, step, width)))
        updates = []
        for x in range(step):
            operand = (turned[x] * out_gain).astype(jnp.bfloat16)
            projected = jnp.dot(out_weights, operand, preferred_element_type=jnp.float32)
            updates.append((gates[start + x] * projected)[None])
        stacked = swap_major(jnp.concatenate(updates, axis=0))
        out_ref[:, pl.ds(start, step)] = stacked.astype(jnp.bfloat16)

    for swap in swaps:
        swap.wait_send()
    for copy in (*edge_copies.values(), *tri_copies.values(), *relays):
        copy.wait_send()


def fused_device(
    rows, pair_act, in_gain, left_proj, left_gate, right_proj, right_gate, out_gate, out_gain, out_proj
):
    half, depth, width = pair_act.shape
    hidden = left_proj.shape[1]
    block = hidden // rows
    channels = 2 * half
    anywhere = pl.BlockSpec(memory_space=pl.ANY)
    local = pl.BlockSpec(memory_space=pltpu.VMEM)
    bf16 = jnp.bfloat16
    dma = pltpu.SemaphoreType.DMA
    return pl.pallas_call(
        functools.partial(fused_kernel, rows),
        out_shape=jax.ShapeDtypeStruct(pair_act.shape, bf16),
        in_specs=[anywhere, local] + [anywhere] * 5 + [local, anywhere],
        out_specs=local,
        scratch_shapes=[
            pltpu.VMEM((2, half, depth, width), bf16),
            pltpu.VMEM((2, 2, half, width), jnp.float32),
            pltpu.VMEM((6 * hidden, channels), bf16),
            pltpu.VMEM((depth, channels, width), bf16),
            pltpu.VMEM((depth, hidden, width), jnp.float32),
            pltpu.VMEM((rows, depth, 2 * block, width), bf16),
            pltpu.VMEM((rows, depth, 2 * block, width), bf16),
            pltpu.VMEM((2 * block, rows * depth, width), bf16),
            pltpu.VMEM((rows, block, depth, width), bf16),
            pltpu.VMEM((2, rows, block, depth, width), bf16),
            dma((7,)),
            dma((2,)),
            dma((2,)),
            dma((rows,)),
            dma((rows,)),
            dma((rows,)),
            dma((rows,)),
            dma((rows,)),
            dma((rows,)),
        ],
        compiler_params=pltpu.CompilerParams(collective_id=0, has_side_effects=True),
        name="triangle",
    )(
        pair_act,
        in_gain[None],
        left_proj.T,
        left_gate.T,
        right_proj.T,
        right_gate.T,
        out_gate.T,
        out_gain[None],
        out_proj.T,
    )


def dispatch(sizes, *args):
    half, depth, width = args[0].shape
    hidden = args[2].shape[1]
    rows = sizes["row"]
    fits = (
        sizes["col"] == 1
        and sizes["ch"] == 2
        and width == rows * depth
        and half == hidden
        and hidden % (8 * rows) == 0
        and depth % 16 == 0
        and width % 128 == 0
    )
    if fits:
        return fused_device(rows, *args)
    return per_device(*args)


def solution(mesh):
    return jax.shard_map(
        functools.partial(dispatch, dict(mesh.shape)),
        mesh=mesh,
        in_specs=(
            P("ch", ("grp", "row"), "col"),
            P("ch"),
            P(None, "ch"),
            P(None, "ch"),
            P(None, "ch"),
            P(None, "ch"),
            P(None, "ch"),
            P("ch"),
            P(None, "ch"),
        ),
        out_specs=P("ch", ("grp", "row"), "col"),
        check_vma=False,
    )
```

```python
import functools

import jax
import jax.numpy as jnp
from jax import lax
from jax.experimental import pallas as pl
from jax.experimental.pallas import tpu as pltpu
from jax.sharding import PartitionSpec as P


def spread_2(value, axis, source):
    kept = jnp.where(lax.axis_index(axis) == source, value, 0).astype(value.dtype)
    return lax.psum(kept, axis)


def moments(values, channel_count):
    first_sums, squares = lax.psum(
        (jnp.sum(values, axis=0), jnp.sum(values * values, axis=0)), "ch"
    )
    average = first_sums / channel_count
    spread = squares / channel_count - average * average
    centred = values - average[None]
    return centred * lax.rsqrt(spread + 1e-05)[None]


def per_device(
    pair_act, in_gain, left_proj, left_gate, right_proj, right_gate, out_gate, out_gain, out_proj
):
    row_count = pair_act.shape[1]
    col_count = pair_act.shape[2]
    hidden = left_proj.shape[1]
    fan_out = col_count // row_count
    normed = (
        moments(pair_act.astype(jnp.float32), pair_act.shape[0] * lax.axis_size("ch"))
        * in_gain[:, None, None]
    ).astype(jnp.bfloat16)
    whole = lax.all_gather(normed, "ch", axis=0, tiled=True)
    left_weights = jnp.concatenate((left_proj, left_gate), axis=1)
    left_lifted = jnp.einsum("cxy,cn->nyx", whole, left_weights, preferred_element_type=jnp.float32)
    left_edge = (jax.nn.sigmoid(left_lifted[hidden:]) * left_lifted[:hidden]).astype(jnp.bfloat16)
    other_weights = jnp.concatenate((right_proj, right_gate, out_gate), axis=1)
    other_lifted = jnp.einsum(
        "cxy,cn->nxy", whole, other_weights, preferred_element_type=jnp.float32
    )
    right_edge = (jax.nn.sigmoid(other_lifted[hidden : 2 * hidden]) * other_lifted[:hidden]).astype(
        jnp.bfloat16
    )
    gate_map = jax.nn.sigmoid(other_lifted[2 * hidden :])
    blocks = left_edge.reshape(hidden, fan_out, row_count, row_count)
    outgoing = jnp.tile(blocks, (1, lax.axis_size("row") // fan_out, 1, 1))
    arrived = lax.all_to_all(outgoing, "row", split_axis=1, concat_axis=3, tiled=True)
    left_panel = arrived.reshape(hidden, row_count, -1)
    left_panel = spread_2(left_panel, "col", lax.axis_index("row") // fan_out)
    tri_sum = jnp.einsum(
        "hik,hkj->hij",
        left_panel,
        lax.all_gather(right_edge, "row", axis=1, tiled=True),
        preferred_element_type=jnp.float32,
    )
    mid_norm = (moments(tri_sum, hidden * lax.axis_size("ch")) * out_gain[:, None, None]).astype(
        jnp.bfloat16
    )
    all_mid = lax.all_gather(mid_norm, "ch", axis=0, tiled=True)
    projected = jnp.einsum("hxy,hc->cxy", all_mid, out_proj, preferred_element_type=jnp.float32)
    return (gate_map * projected).astype(jnp.bfloat16)


MESH = pl.DeviceIdType.MESH


def swap_major(values):
    return jnp.swapaxes(values, 0, 1)


def spread_gain(gain, lanes):
    return jnp.broadcast_to(gain, (lanes, gain.shape[1])).T


def centred_unit(values, gain):
    count = values.shape[0]
    average = jnp.sum(values, axis=0, keepdims=True) / count
    centred = values - average
    spread = jnp.sum(centred * centred, axis=0, keepdims=True) / count
    return (centred * lax.rsqrt(spread + 1e-05) * gain).astype(jnp.bfloat16)


def fused_kernel(
    rows,
    act_ref,
    gain_ref,
    lp_ref,
    lg_ref,
    rp_ref,
    rg_ref,
    og_ref,
    gain2_ref,
    op_ref,
    out_ref,
    raw,
    act,
    gains,
    weights,
    edge_weights,
    normed,
    gates,
    outbox,
    inbox,
    edges,
    tri_out,
    tri_in,
    mid,
    load_sem,
    pair_send,
    pair_recv,
    lr_send,
    lr_recv,
    tri_send,
    tri_recv,
    relay_send,
    relay_recv,
):
    me = lax.axis_index("row")
    core = lax.axis_index("ch")
    other = 1 - core
    half, depth, width = act_ref.shape
    hidden = lp_ref.shape[0]
    part = hidden // rows // 2
    partner = {"ch": other}
    peers = [lax.rem(me + d, rows) for d in range(rows)]
    sources = [lax.rem(me + rows - d, rows) for d in range(rows)]
    order = sorted(range(1, rows), key=lambda d: -min(d, rows - d))
    step = depth // 2
    halves = (pl.ds(0, step), pl.ds(step, step))

    loads = [pltpu.make_async_copy(act_ref, raw, load_sem.at[0])]
    for n, ref in enumerate((lp_ref, lg_ref, rp_ref, rg_ref, og_ref, op_ref)):
        loads.append(pltpu.make_async_copy(ref, weights.at[n], load_sem.at[n + 1]))
    for load in loads:
        load.start()
    barrier = pltpu.get_barrier_semaphore()
    pl.semaphore_signal(barrier, inc=1, device_id=partner, device_id_type=MESH)
    for d in range(1, rows):
        pl.semaphore_signal(barrier, inc=1, device_id={"row": peers[d]}, device_id_type=MESH)
    gains[core, 0] = spread_gain(gain_ref[...], width)
    gains[core, 1] = spread_gain(gain2_ref[...], width)
    loads[0].wait()
    for n in range(2):
        turned = swap_major(raw[:, halves[n]].astype(jnp.float32))
        act[core, halves[n]] = turned.astype(jnp.bfloat16)

    def to_partner(ref, n):
        return pltpu.make_async_remote_copy(
            src_ref=ref,
            dst_ref=ref,
            send_sem=pair_send.at[n],
            recv_sem=pair_recv.at[n],
            device_id=partner,
            device_id_type=MESH,
        )

    pl.semaphore_wait(barrier, rows)
    swaps = [
        to_partner(gains.at[core], 2),
        to_partner(act.at[core, halves[0]], 0),
        to_partner(act.at[core, halves[1]], 1),
    ]
    for swap in swaps:
        swap.start()
    for load in loads[1:]:
        load.wait()
    for n in range(2):
        first = weights[n].astype(jnp.float32).reshape(rows, 2, part, 2 * half)
        second = weights[n + 2].astype(jnp.float32).reshape(rows, 2, part, 2 * half)
        joined = jnp.concatenate((first, second), axis=2)
        edge_weights[n] = joined.reshape(2 * hidden, 2 * half).astype(jnp.bfloat16)

    def edge_copy(n, src, dst, d):
        return pltpu.make_async_remote_copy(
            src_ref=src,
            dst_ref=dst,
            send_sem=lr_send.at[n, d],
            recv_sem=lr_recv.at[n, d],
            device_id={"row": peers[d]},
            device_id_type=MESH,
        )

    first_copies = [
        {
            d: edge_copy(n, outbox.at[0, peers[d], halves[n]], inbox.at[0, me, halves[n]], d)
            for d in order
        }
        for n in range(2)
    ]
    last_copies = {d: edge_copy(2, outbox.at[1, peers[d]], inbox.at[1, me], d) for d in order}

    swaps[0].wait_recv()
    in_gain = gains[:, 0].reshape(2 * half, width)
    lift_weights = edge_weights[...].reshape(4 * hidden, 2 * half)
    for n in range(2):
        swaps[1 + n].wait_recv()
        for x in range(n * step, (n + 1) * step):
            values = act[:, x].astype(jnp.float32).reshape(2 * half, width)
            operand = centred_unit(values, in_gain)
            normed[x] = operand
            lifted = jnp.dot(lift_weights, operand, preferred_element_type=jnp.float32)
            both = jax.nn.sigmoid(lifted[2 * hidden :]) * lifted[: 2 * hidden]
            both = both.reshape(rows, 2, 2 * part, width).astype(jnp.bfloat16)
            outbox[0, :, x] = both[:, 0]
            outbox[1, :, x] = both[:, 1]
        for d in order:
            first_copies[n][d].start()
    for d in order:
        last_copies[d].start()

    def take_edges(n, box, source):
        turned = swap_major(box.astype(jnp.float32)).astype(jnp.bfloat16)
        edges[n, :, pl.ds(pl.multiple_of(source * depth, depth), depth)] = turned

    for n in range(2):
        take_edges(n, outbox[n, me], me)
    gate_weights = weights[4]
    for x in range(depth):
        gates[x] = jax.nn.sigmoid(
            jnp.dot(gate_weights, normed[x], preferred_element_type=jnp.float32)
        )

    def tri_copy(n, d):
        return pltpu.make_async_remote_copy(
            src_ref=tri_out.at[peers[d], n],
            dst_ref=tri_in.at[me, n],
            send_sem=tri_send.at[n, d],
            recv_sem=tri_recv.at[n, d],
            device_id={"row": peers[d]},
            device_id_type=MESH,
        )

    tri_copies = [{d: tri_copy(n, d) for d in order} for n in range(2)]
    for n in range(2):
        for d in order:
            if n == 0:
                first_copies[0][d].wait_recv()
                first_copies[1][d].wait_recv()
            else:
                last_copies[d].wait_recv()
            take_edges(n, inbox[n, sources[d]], sources[d])
        for h in range(part):
            tri_sum = lax.dot_general(
                edges[n, h],
                edges[n, part + h],
                (((0,), (0,)), ((), ())),
                preferred_element_type=jnp.float32,
            )
            tri_out[:, n, h] = tri_sum.astype(jnp.bfloat16).reshape(rows, depth, width)
        for d in order:
            tri_copies[n][d].start()

    def relay(source, d):
        return pltpu.make_async_remote_copy(
            src_ref=mid.at[core, source],
            dst_ref=mid.at[core, source],
            send_sem=relay_send.at[d],
            recv_sem=relay_recv.at[d],
            device_id=partner,
            device_id_type=MESH,
        )

    def take_mid(block, source):
        block = block.astype(jnp.float32).reshape(2 * part, depth, width)
        mid[core, source] = swap_major(block).astype(jnp.bfloat16)

    take_mid(tri_out[me], me)
    relays = [relay(me, 0)]
    relays[0].start()
    for d in order:
        for n in range(2):
            tri_copies[n][d].wait_recv()
        take_mid(tri_in[sources[d]], sources[d])
        relays.append(relay(sources[d], d))
        relays[-1].start()
    for copy in relays:
        copy.wait_recv()

    out_gain = gains[:, 1].reshape(2 * half, width)
    out_weights = weights[5]
    for start in range(0, depth, step):
        updates = []
        for x in range(start, start + step):
            values = mid[:, :, x].astype(jnp.float32).reshape(2 * hidden, width)
            operand = centred_unit(values, out_gain)
            projected = jnp.dot(out_weights, operand, preferred_element_type=jnp.float32)
            updates.append((gates[x] * projected)[None])
        stacked = swap_major(jnp.concatenate(updates, axis=0))
        out_ref[:, pl.ds(start, step)] = stacked.astype(jnp.bfloat16)

    for swap in swaps:
        swap.wait_send()
    for copies in (*first_copies, last_copies, *tri_copies):
        for copy in copies.values():
            copy.wait_send()
    for copy in relays:
        copy.wait_send()


def fused_device(
    rows, pair_act, in_gain, left_proj, left_gate, right_proj, right_gate, out_gate, out_gain, out_proj
):
    half, depth, width = pair_act.shape
    hidden = left_proj.shape[1]
    part = hidden // rows // 2
    channels = 2 * half
    anywhere = pl.BlockSpec(memory_space=pl.ANY)
    local = pl.BlockSpec(memory_space=pltpu.VMEM)
    bf16 = jnp.bfloat16
    dma = pltpu.SemaphoreType.DMA
    return pl.pallas_call(
        functools.partial(fused_kernel, rows),
        out_shape=pltpu.VMEM(pair_act.shape, bf16),
        in_specs=[anywhere, local] + [anywhere] * 5 + [local, anywhere],
        out_specs=local,
        scratch_shapes=[
            pltpu.VMEM((half, depth, width), bf16),
            pltpu.VMEM((2, depth, half, width), bf16),
            pltpu.VMEM((2, 2, half, width), jnp.float32),
            pltpu.VMEM((6, hidden, channels), bf16),
            pltpu.VMEM((2, 2 * hidden, channels), bf16),
            pltpu.VMEM((depth, channels, width), bf16),
            pltpu.VMEM((depth, hidden, width), jnp.float32),
            pltpu.VMEM((2, rows, depth, 2 * part, width), bf16),
            pltpu.VMEM((2, rows, depth, 2 * part, width), bf16),
            pltpu.VMEM((2, 2 * part, rows * depth, width), bf16),
            pltpu.VMEM((rows, 2, part, depth, width), bf16),
            pltpu.VMEM((rows, 2, part, depth, width), bf16),
            pltpu.VMEM((2, rows, depth, 2 * part, width), bf16),
            dma((7,)),
            dma((3,)),
            dma((3,)),
            dma((3, rows)),
            dma((3, rows)),
            dma((2, rows)),
            dma((2, rows)),
            dma((rows,)),
            dma((rows,)),
        ],
        compiler_params=pltpu.CompilerParams(collective_id=0, has_side_effects=True),
        name="triangle",
    )(
        pair_act,
        in_gain[None],
        left_proj.T,
        left_gate.T,
        right_proj.T,
        right_gate.T,
        out_gate.T,
        out_gain[None],
        out_proj.T,
    )


def dispatch(sizes, *args):
    half, depth, width = args[0].shape
    hidden = args[2].shape[1]
    rows = sizes["row"]
    fits = (
        sizes["col"] == 1
        and sizes["ch"] == 2
        and width == rows * depth
        and half == hidden
        and hidden % (8 * rows) == 0
        and depth % 16 == 0
        and width % 128 == 0
    )
    if fits:
        return fused_device(rows, *args)
    return per_device(*args)


def solution(mesh):
    return jax.shard_map(
        functools.partial(dispatch, dict(mesh.shape)),
        mesh=mesh,
        in_specs=(
            P("ch", ("grp", "row"), "col"),
            P("ch"),
            P(None, "ch"),
            P(None, "ch"),
            P(None, "ch"),
            P(None, "ch"),
            P(None, "ch"),
            P("ch"),
            P(None, "ch"),
        ),
        out_specs=P("ch", ("grp", "row"), "col"),
        check_vma=False,
    )
```

```python
import functools

import jax
import jax.numpy as jnp
from jax import lax
from jax.experimental import pallas as pl
from jax.experimental.pallas import tpu as pltpu
from jax.sharding import PartitionSpec as P


def spread_2(value, axis, source):
    kept = jnp.where(lax.axis_index(axis) == source, value, 0).astype(value.dtype)
    return lax.psum(kept, axis)


def moments(values, channel_count):
    first_sums, squares = lax.psum(
        (jnp.sum(values, axis=0), jnp.sum(values * values, axis=0)), "ch"
    )
    average = first_sums / channel_count
    spread = squares / channel_count - average * average
    centred = values - average[None]
    return centred * lax.rsqrt(spread + 1e-05)[None]


def per_device(
    pair_act, in_gain, left_proj, left_gate, right_proj, right_gate, out_gate, out_gain, out_proj
):
    row_count = pair_act.shape[1]
    col_count = pair_act.shape[2]
    hidden = left_proj.shape[1]
    fan_out = col_count // row_count
    normed = (
        moments(pair_act.astype(jnp.float32), pair_act.shape[0] * lax.axis_size("ch"))
        * in_gain[:, None, None]
    ).astype(jnp.bfloat16)
    whole = lax.all_gather(normed, "ch", axis=0, tiled=True)
    left_weights = jnp.concatenate((left_proj, left_gate), axis=1)
    left_lifted = jnp.einsum("cxy,cn->nyx", whole, left_weights, preferred_element_type=jnp.float32)
    left_edge = (jax.nn.sigmoid(left_lifted[hidden:]) * left_lifted[:hidden]).astype(jnp.bfloat16)
    other_weights = jnp.concatenate((right_proj, right_gate, out_gate), axis=1)
    other_lifted = jnp.einsum(
        "cxy,cn->nxy", whole, other_weights, preferred_element_type=jnp.float32
    )
    right_edge = (jax.nn.sigmoid(other_lifted[hidden : 2 * hidden]) * other_lifted[:hidden]).astype(
        jnp.bfloat16
    )
    gate_map = jax.nn.sigmoid(other_lifted[2 * hidden :])
    blocks = left_edge.reshape(hidden, fan_out, row_count, row_count)
    outgoing = jnp.tile(blocks, (1, lax.axis_size("row") // fan_out, 1, 1))
    arrived = lax.all_to_all(outgoing, "row", split_axis=1, concat_axis=3, tiled=True)
    left_panel = arrived.reshape(hidden, row_count, -1)
    left_panel = spread_2(left_panel, "col", lax.axis_index("row") // fan_out)
    tri_sum = jnp.einsum(
        "hik,hkj->hij",
        left_panel,
        lax.all_gather(right_edge, "row", axis=1, tiled=True),
        preferred_element_type=jnp.float32,
    )
    mid_norm = (moments(tri_sum, hidden * lax.axis_size("ch")) * out_gain[:, None, None]).astype(
        jnp.bfloat16
    )
    all_mid = lax.all_gather(mid_norm, "ch", axis=0, tiled=True)
    projected = jnp.einsum("hxy,hc->cxy", all_mid, out_proj, preferred_element_type=jnp.float32)
    return (gate_map * projected).astype(jnp.bfloat16)


MESH = pl.DeviceIdType.MESH


def swap_major(values):
    return jnp.swapaxes(values, 0, 1)


def spread_gain(gain, lanes):
    return jnp.broadcast_to(gain, (lanes, gain.shape[1])).T


def centred_unit(values, gain):
    count = values.shape[0]
    average = jnp.sum(values, axis=0, keepdims=True) / count
    centred = values - average
    spread = jnp.sum(centred * centred, axis=0, keepdims=True) / count
    return (centred * lax.rsqrt(spread + 1e-05) * gain).astype(jnp.bfloat16)


def fused_kernel(
    rows,
    act_ref,
    gain_ref,
    lp_ref,
    lg_ref,
    rp_ref,
    rg_ref,
    og_ref,
    gain2_ref,
    op_ref,
    out_ref,
    raw,
    act,
    gains,
    weights,
    edge_weights,
    normed,
    gates,
    outbox,
    inbox,
    edges,
    tri_out,
    tri_in,
    mid,
    load_sem,
    pair_send,
    pair_recv,
    lr_send,
    lr_recv,
    tri_send,
    tri_recv,
    relay_send,
    relay_recv,
    up_sem,
    down_sem,
):
    me = lax.axis_index("row")
    core = lax.axis_index("ch")
    other = 1 - core
    half, depth, width = act_ref.shape
    hidden = lp_ref.shape[0]
    part = hidden // rows // 2
    partner = {"ch": other}
    peers = [lax.rem(me + d, rows) for d in range(rows)]
    sources = [lax.rem(me + rows - d, rows) for d in range(rows)]
    order = sorted(range(1, rows), key=lambda d: -min(d, rows - d))
    step = depth // 2
    halves = (pl.ds(0, step), pl.ds(step, step))

    loads = [pltpu.make_async_copy(act_ref, raw, load_sem.at[0])]
    for n, ref in enumerate((lp_ref, lg_ref, rp_ref, rg_ref, og_ref, op_ref)):
        loads.append(pltpu.make_async_copy(ref, weights.at[n], load_sem.at[n + 1]))
    for load in loads:
        load.start()
    barrier = pltpu.get_barrier_semaphore()
    side = lax.rem(me, 2)
    across, above, below = me + 1 - 2 * side, me + 2, me - 2
    has_above, has_below = me + 2 < rows, me >= 2

    def greet(semaphore, device):
        pl.semaphore_signal(semaphore, inc=1, device_id=device, device_id_type=MESH)

    def pass_up():
        @pl.when(has_below)
        def _():
            pl.semaphore_wait(up_sem, 1)

        @pl.when(jnp.logical_and(has_below, has_above))
        def _():
            greet(up_sem, {"row": above})

    def pass_down():
        @pl.when(has_above)
        def _():
            pl.semaphore_wait(down_sem, 1)

        @pl.when(jnp.logical_and(has_below, has_above))
        def _():
            greet(down_sem, {"row": below})

    greet(barrier, partner)
    greet(barrier, {"row": across})

    @pl.when(has_above)
    def _():
        greet(barrier, {"row": above})

    @pl.when(has_below)
    def _():
        greet(barrier, {"row": below})

    gains[core, 0] = spread_gain(gain_ref[...], width)
    gains[core, 1] = spread_gain(gain2_ref[...], width)
    loads[0].wait()
    for n in range(2):
        turned = swap_major(raw[:, halves[n]].astype(jnp.float32))
        act[core, halves[n]] = turned.astype(jnp.bfloat16)

    def to_partner(ref, n):
        return pltpu.make_async_remote_copy(
            src_ref=ref,
            dst_ref=ref,
            send_sem=pair_send.at[n],
            recv_sem=pair_recv.at[n],
            device_id=partner,
            device_id_type=MESH,
        )

    pl.semaphore_wait(barrier, 2 + has_above.astype(jnp.int32) + has_below.astype(jnp.int32))

    @pl.when(jnp.logical_not(has_below))
    def _():
        greet(up_sem, {"row": above})

    @pl.when(jnp.logical_not(has_above))
    def _():
        greet(down_sem, {"row": below})

    swaps = [
        to_partner(gains.at[core], 2),
        to_partner(act.at[core, halves[0]], 0),
        to_partner(act.at[core, halves[1]], 1),
    ]
    for swap in swaps:
        swap.start()

    @pl.when(2 * me < rows)
    def _():
        pass_up()
        pass_down()

    @pl.when(2 * me >= rows)
    def _():
        pass_down()
        pass_up()

    for load in loads[1:]:
        load.wait()
    for n in range(2):
        first = weights[n].astype(jnp.float32).reshape(rows, 2, part, 2 * half)
        second = weights[n + 2].astype(jnp.float32).reshape(rows, 2, part, 2 * half)
        joined = jnp.concatenate((first, second), axis=2)
        edge_weights[n] = joined.reshape(2 * hidden, 2 * half).astype(jnp.bfloat16)

    def edge_copy(n, src, dst, d):
        return pltpu.make_async_remote_copy(
            src_ref=src,
            dst_ref=dst,
            send_sem=lr_send.at[n, d],
            recv_sem=lr_recv.at[n, d],
            device_id={"row": peers[d]},
            device_id_type=MESH,
        )

    first_copies = [
        {
            d: edge_copy(n, outbox.at[0, peers[d], halves[n]], inbox.at[0, me, halves[n]], d)
            for d in order
        }
        for n in range(2)
    ]
    last_copies = {d: edge_copy(2, outbox.at[1, peers[d]], inbox.at[1, me], d) for d in order}

    swaps[0].wait_recv()
    in_gain = gains[:, 0].reshape(2 * half, width)
    lift_weights = edge_weights[...].reshape(4 * hidden, 2 * half)
    for n in range(2):
        swaps[1 + n].wait_recv()
        for x in range(n * step, (n + 1) * step):
            values = act[:, x].astype(jnp.float32).reshape(2 * half, width)
            operand = centred_unit(values, in_gain)
            normed[x] = operand
            lifted = jnp.dot(lift_weights, operand, preferred_element_type=jnp.float32)
            both = jax.nn.sigmoid(lifted[2 * hidden :]) * lifted[: 2 * hidden]
            both = both.reshape(rows, 2, 2 * part, width).astype(jnp.bfloat16)
            outbox[0, :, x] = both[:, 0]
            outbox[1, :, x] = both[:, 1]
        for d in order:
            first_copies[n][d].start()
    for d in order:
        last_copies[d].start()

    def take_edges(n, box, source):
        turned = swap_major(box.astype(jnp.float32)).astype(jnp.bfloat16)
        edges[n, :, pl.ds(pl.multiple_of(source * depth, depth), depth)] = turned

    for n in range(2):
        take_edges(n, outbox[n, me], me)
    gate_weights = weights[4]
    for x in range(depth):
        gates[x] = jax.nn.sigmoid(
            jnp.dot(gate_weights, normed[x], preferred_element_type=jnp.float32)
        )

    def tri_copy(n, d):
        return pltpu.make_async_remote_copy(
            src_ref=tri_out.at[peers[d], n],
            dst_ref=tri_in.at[me, n],
            send_sem=tri_send.at[n, d],
            recv_sem=tri_recv.at[n, d],
            device_id={"row": peers[d]},
            device_id_type=MESH,
        )

    tri_copies = [{d: tri_copy(n, d) for d in order} for n in range(2)]
    for n in range(2):
        for d in order:
            if n == 0:
                first_copies[0][d].wait_recv()
                first_copies[1][d].wait_recv()
            else:
                last_copies[d].wait_recv()
            take_edges(n, inbox[n, sources[d]], sources[d])
        for h in range(part):
            tri_sum = lax.dot_general(
                edges[n, h],
                edges[n, part + h],
                (((0,), (0,)), ((), ())),
                preferred_element_type=jnp.float32,
            )
            tri_out[:, n, h] = tri_sum.astype(jnp.bfloat16).reshape(rows, depth, width)
        for d in order:
            tri_copies[n][d].start()

    def relay(source, d):
        return pltpu.make_async_remote_copy(
            src_ref=mid.at[core, source],
            dst_ref=mid.at[core, source],
            send_sem=relay_send.at[d],
            recv_sem=relay_recv.at[d],
            device_id=partner,
            device_id_type=MESH,
        )

    def take_mid(block, source):
        block = block.astype(jnp.float32).reshape(2 * part, depth, width)
        mid[core, source] = swap_major(block).astype(jnp.bfloat16)

    take_mid(tri_out[me], me)
    relays = [relay(me, 0)]
    relays[0].start()
    for d in order:
        for n in range(2):
            tri_copies[n][d].wait_recv()
        take_mid(tri_in[sources[d]], sources[d])
        relays.append(relay(sources[d], d))
        relays[-1].start()
    for copy in relays:
        copy.wait_recv()

    out_gain = gains[:, 1].reshape(2 * half, width)
    out_weights = weights[5]
    for start in range(0, depth, step):
        updates = []
        for x in range(start, start + step):
            values = mid[:, :, x].astype(jnp.float32).reshape(2 * hidden, width)
            operand = centred_unit(values, out_gain)
            projected = jnp.dot(out_weights, operand, preferred_element_type=jnp.float32)
            updates.append((gates[x] * projected)[None])
        stacked = swap_major(jnp.concatenate(updates, axis=0))
        out_ref[:, pl.ds(start, step)] = stacked.astype(jnp.bfloat16)

    for swap in swaps:
        swap.wait_send()
    for copies in (*first_copies, last_copies, *tri_copies):
        for copy in copies.values():
            copy.wait_send()
    for copy in relays:
        copy.wait_send()


def fused_device(
    rows, pair_act, in_gain, left_proj, left_gate, right_proj, right_gate, out_gate, out_gain, out_proj
):
    half, depth, width = pair_act.shape
    hidden = left_proj.shape[1]
    part = hidden // rows // 2
    channels = 2 * half
    anywhere = pl.BlockSpec(memory_space=pl.ANY)
    local = pl.BlockSpec(memory_space=pltpu.VMEM)
    bf16 = jnp.bfloat16
    dma = pltpu.SemaphoreType.DMA
    return pl.pallas_call(
        functools.partial(fused_kernel, rows),
        out_shape=pltpu.VMEM(pair_act.shape, bf16),
        in_specs=[anywhere, local] + [anywhere] * 5 + [local, anywhere],
        out_specs=local,
        scratch_shapes=[
            pltpu.VMEM((half, depth, width), bf16),
            pltpu.VMEM((2, depth, half, width), bf16),
            pltpu.VMEM((2, 2, half, width), jnp.float32),
            pltpu.VMEM((6, hidden, channels), bf16),
            pltpu.VMEM((2, 2 * hidden, channels), bf16),
            pltpu.VMEM((depth, channels, width), bf16),
            pltpu.VMEM((depth, hidden, width), jnp.float32),
            pltpu.VMEM((2, rows, depth, 2 * part, width), bf16),
            pltpu.VMEM((2, rows, depth, 2 * part, width), bf16),
            pltpu.VMEM((2, 2 * part, rows * depth, width), bf16),
            pltpu.VMEM((rows, 2, part, depth, width), bf16),
            pltpu.VMEM((rows, 2, part, depth, width), bf16),
            pltpu.VMEM((2, rows, depth, 2 * part, width), bf16),
            dma((7,)),
            dma((3,)),
            dma((3,)),
            dma((3, rows)),
            dma((3, rows)),
            dma((2, rows)),
            dma((2, rows)),
            dma((rows,)),
            dma((rows,)),
            pltpu.SemaphoreType.REGULAR,
            pltpu.SemaphoreType.REGULAR,
        ],
        compiler_params=pltpu.CompilerParams(collective_id=0, has_side_effects=True),
        name="triangle",
    )(
        pair_act,
        in_gain[None],
        left_proj.T,
        left_gate.T,
        right_proj.T,
        right_gate.T,
        out_gate.T,
        out_gain[None],
        out_proj.T,
    )


def dispatch(sizes, *args):
    half, depth, width = args[0].shape
    hidden = args[2].shape[1]
    rows = sizes["row"]
    fits = (
        sizes["col"] == 1
        and sizes["ch"] == 2
        and width == rows * depth
        and half == hidden
        and hidden % (8 * rows) == 0
        and depth % 16 == 0
        and rows % 2 == 0
        and rows >= 4
        and width % 128 == 0
    )
    if fits:
        return fused_device(rows, *args)
    return per_device(*args)


def solution(mesh):
    return jax.shard_map(
        functools.partial(dispatch, dict(mesh.shape)),
        mesh=mesh,
        in_specs=(
            P("ch", ("grp", "row"), "col"),
            P("ch"),
            P(None, "ch"),
            P(None, "ch"),
            P(None, "ch"),
            P(None, "ch"),
            P(None, "ch"),
            P("ch"),
            P(None, "ch"),
        ),
        out_specs=P("ch", ("grp", "row"), "col"),
        check_vma=False,
    )
```

```python
import functools

import jax
import jax.numpy as jnp
from jax import lax
from jax.experimental import pallas as pl
from jax.experimental.pallas import tpu as pltpu
from jax.sharding import PartitionSpec as P


def spread_2(value, axis, source):
    kept = jnp.where(lax.axis_index(axis) == source, value, 0).astype(value.dtype)
    return lax.psum(kept, axis)


def moments(values, channel_count):
    first_sums, squares = lax.psum(
        (jnp.sum(values, axis=0), jnp.sum(values * values, axis=0)), "ch"
    )
    average = first_sums / channel_count
    spread = squares / channel_count - average * average
    centred = values - average[None]
    return centred * lax.rsqrt(spread + 1e-05)[None]


def per_device(
    pair_act, in_gain, left_proj, left_gate, right_proj, right_gate, out_gate, out_gain, out_proj
):
    row_count = pair_act.shape[1]
    col_count = pair_act.shape[2]
    hidden = left_proj.shape[1]
    fan_out = col_count // row_count
    normed = (
        moments(pair_act.astype(jnp.float32), pair_act.shape[0] * lax.axis_size("ch"))
        * in_gain[:, None, None]
    ).astype(jnp.bfloat16)
    whole = lax.all_gather(normed, "ch", axis=0, tiled=True)
    left_weights = jnp.concatenate((left_proj, left_gate), axis=1)
    left_lifted = jnp.einsum("cxy,cn->nyx", whole, left_weights, preferred_element_type=jnp.float32)
    left_edge = (jax.nn.sigmoid(left_lifted[hidden:]) * left_lifted[:hidden]).astype(jnp.bfloat16)
    other_weights = jnp.concatenate((right_proj, right_gate, out_gate), axis=1)
    other_lifted = jnp.einsum(
        "cxy,cn->nxy", whole, other_weights, preferred_element_type=jnp.float32
    )
    right_edge = (jax.nn.sigmoid(other_lifted[hidden : 2 * hidden]) * other_lifted[:hidden]).astype(
        jnp.bfloat16
    )
    gate_map = jax.nn.sigmoid(other_lifted[2 * hidden :])
    blocks = left_edge.reshape(hidden, fan_out, row_count, row_count)
    outgoing = jnp.tile(blocks, (1, lax.axis_size("row") // fan_out, 1, 1))
    arrived = lax.all_to_all(outgoing, "row", split_axis=1, concat_axis=3, tiled=True)
    left_panel = arrived.reshape(hidden, row_count, -1)
    left_panel = spread_2(left_panel, "col", lax.axis_index("row") // fan_out)
    tri_sum = jnp.einsum(
        "hik,hkj->hij",
        left_panel,
        lax.all_gather(right_edge, "row", axis=1, tiled=True),
        preferred_element_type=jnp.float32,
    )
    mid_norm = (moments(tri_sum, hidden * lax.axis_size("ch")) * out_gain[:, None, None]).astype(
        jnp.bfloat16
    )
    all_mid = lax.all_gather(mid_norm, "ch", axis=0, tiled=True)
    projected = jnp.einsum("hxy,hc->cxy", all_mid, out_proj, preferred_element_type=jnp.float32)
    return (gate_map * projected).astype(jnp.bfloat16)


MESH = pl.DeviceIdType.MESH


def swap_major(values):
    return jnp.swapaxes(values, 0, 1)


def spread_gain(gain, lanes):
    return jnp.broadcast_to(gain, (lanes, gain.shape[1])).T


def centred_unit(values, gain):
    count = values.shape[0]
    average = jnp.sum(values, axis=0, keepdims=True) / count
    centred = values - average
    spread = jnp.sum(centred * centred, axis=0, keepdims=True) / count
    return (centred * lax.rsqrt(spread + 1e-05) * gain).astype(jnp.bfloat16)


def fused_kernel(
    rows,
    act_ref,
    gain_ref,
    lp_ref,
    lg_ref,
    rp_ref,
    rg_ref,
    og_ref,
    gain2_ref,
    op_ref,
    out_ref,
    raw,
    act,
    gains,
    weights,
    edge_weights,
    normed,
    gates,
    outbox,
    inbox,
    edges,
    tri_out,
    tri_in,
    mid,
    near_in,
    near_edges,
    part_sums,
    part_out,
    part_in,
    near_out,
    back_in,
    load_sem,
    pair_send,
    pair_recv,
    lr_send,
    lr_recv,
    tri_send,
    tri_recv,
    relay_send,
    relay_recv,
    near_send,
    near_recv,
    part_send,
    part_recv,
    back_send,
    back_recv,
):
    me = lax.axis_index("row")
    core = lax.axis_index("ch")
    other = 1 - core
    half, depth, width = act_ref.shape
    hidden = lp_ref.shape[0]
    part = hidden // rows // 2
    partner = {"ch": other}
    peers = [lax.rem(me + d, rows) for d in range(rows)]
    sources = [lax.rem(me + rows - d, rows) for d in range(rows)]
    order = sorted(range(1, rows), key=lambda d: -min(d, rows - d))
    step = depth // 2
    near = rows // 2
    base = me // near * near
    place = me - base
    far_base = near - base
    mates = [base + lax.rem(place + d, near) for d in range(near)]
    mate_places = [lax.rem(place + d, near) for d in range(near)]
    from_places = [lax.rem(place + near - d, near) for d in range(near)]
    halves = (pl.ds(0, step), pl.ds(step, step))

    loads = [pltpu.make_async_copy(act_ref, raw, load_sem.at[0])]
    for n, ref in enumerate((lp_ref, lg_ref, rp_ref, rg_ref, og_ref, op_ref)):
        loads.append(pltpu.make_async_copy(ref, weights.at[n], load_sem.at[n + 1]))
    for load in loads:
        load.start()
    barrier = pltpu.get_barrier_semaphore()
    pl.semaphore_signal(barrier, inc=1, device_id=partner, device_id_type=MESH)
    for d in range(1, rows):
        pl.semaphore_signal(barrier, inc=1, device_id={"row": peers[d]}, device_id_type=MESH)
    gains[core, 0] = spread_gain(gain_ref[...], width)
    gains[core, 1] = spread_gain(gain2_ref[...], width)
    loads[0].wait()
    for n in range(2):
        turned = swap_major(raw[:, halves[n]].astype(jnp.float32))
        act[core, halves[n]] = turned.astype(jnp.bfloat16)

    def to_partner(ref, n):
        return pltpu.make_async_remote_copy(
            src_ref=ref,
            dst_ref=ref,
            send_sem=pair_send.at[n],
            recv_sem=pair_recv.at[n],
            device_id=partner,
            device_id_type=MESH,
        )

    pl.semaphore_wait(barrier, rows)
    swaps = [
        to_partner(gains.at[core], 2),
        to_partner(act.at[core, halves[0]], 0),
        to_partner(act.at[core, halves[1]], 1),
    ]
    for swap in swaps:
        swap.start()
    for load in loads[1:]:
        load.wait()
    for n in range(2):
        first = weights[n].astype(jnp.float32).reshape(2, rows, part, 2 * half)
        second = weights[n + 2].astype(jnp.float32).reshape(2, rows, part, 2 * half)
        joined = jnp.concatenate((first, second), axis=2)
        edge_weights[n] = joined.reshape(2 * hidden, 2 * half).astype(jnp.bfloat16)

    def edge_copy(n, src, dst, d):
        return pltpu.make_async_remote_copy(
            src_ref=src,
            dst_ref=dst,
            send_sem=lr_send.at[n, d],
            recv_sem=lr_recv.at[n, d],
            device_id={"row": peers[d]},
            device_id_type=MESH,
        )

    first_copies = [
        {
            d: edge_copy(n, outbox.at[0, peers[d], halves[n]], inbox.at[0, me, halves[n]], d)
            for d in order
        }
        for n in range(2)
    ]

    def mate_copy(src, dst, sends, recvs, d):
        return pltpu.make_async_remote_copy(
            src_ref=src,
            dst_ref=dst,
            send_sem=sends.at[d],
            recv_sem=recvs.at[d],
            device_id={"row": mates[d]},
            device_id_type=MESH,
        )

    near_copies = {
        d: mate_copy(
            outbox.at[1, pl.ds(2 * mate_places[d], 2)],
            near_in.at[place],
            near_send,
            near_recv,
            d,
        )
        for d in range(1, near)
    }

    swaps[0].wait_recv()
    in_gain = gains[:, 0].reshape(2 * half, width)
    lift_weights = edge_weights[...].reshape(4 * hidden, 2 * half)
    for n in range(2):
        swaps[1 + n].wait_recv()
        for x in range(n * step, (n + 1) * step):
            values = act[:, x].astype(jnp.float32).reshape(2 * half, width)
            operand = centred_unit(values, in_gain)
            normed[x] = operand
            lifted = jnp.dot(lift_weights, operand, preferred_element_type=jnp.float32)
            both = jax.nn.sigmoid(lifted[2 * hidden :]) * lifted[: 2 * hidden]
            both = both.reshape(2, rows, 2 * part, width).astype(jnp.bfloat16)
            outbox[0, :, x] = both[0]
            outbox[1, :, x] = both[1]
        if n == 1:
            for copy in near_copies.values():
                copy.start()
        for d in order:
            first_copies[n][d].start()

    def take_edges(box, source):
        turned = swap_major(box.astype(jnp.float32)).astype(jnp.bfloat16)
        edges[:, pl.ds(pl.multiple_of(source * depth, depth), depth)] = turned

    def take_near(boxes, source):
        for n in range(2):
            turned = swap_major(boxes[n].astype(jnp.float32)).astype(jnp.bfloat16)
            near_edges[n, :, pl.ds(pl.multiple_of(source * depth, depth), depth)] = turned

    take_edges(outbox[0, me], me)
    take_near(outbox.at[1, pl.ds(2 * place, 2)], place)
    gate_weights = weights[4]
    for x in range(depth):
        gates[x] = jax.nn.sigmoid(
            jnp.dot(gate_weights, normed[x], preferred_element_type=jnp.float32)
        )

    def contract(first, second):
        return lax.dot_general(
            first, second, (((0,), (0,)), ((), ())), preferred_element_type=jnp.float32
        )

    for d in range(1, near):
        near_copies[d].wait_recv()
        take_near(near_in.at[from_places[d]], from_places[d])
    for n in range(2):
        for h in range(part):
            partial = contract(near_edges[n, h], near_edges[n, part + h])
            part_sums[:, n * part + h] = partial.reshape(2, near * depth, width)
    part_out[...] = part_sums[far_base // near].astype(jnp.bfloat16)
    opposite = pltpu.make_async_remote_copy(
        src_ref=part_out,
        dst_ref=part_in,
        send_sem=part_send.at[0],
        recv_sem=part_recv.at[0],
        device_id={"row": far_base + place},
        device_id_type=MESH,
    )
    opposite.start()

    tri_copies = {
        d: pltpu.make_async_remote_copy(
            src_ref=tri_out.at[peers[d]],
            dst_ref=tri_in.at[me],
            send_sem=tri_send.at[d],
            recv_sem=tri_recv.at[d],
            device_id={"row": peers[d]},
            device_id_type=MESH,
        )
        for d in order
    }
    for d in order:
        first_copies[0][d].wait_recv()
        first_copies[1][d].wait_recv()
        take_edges(inbox[0, sources[d]], sources[d])
    for h in range(part):
        tri_sum = contract(edges[h], edges[part + h])
        tri_out[:, h] = tri_sum.astype(jnp.bfloat16).reshape(rows, depth, width)
    for d in order:
        tri_copies[d].start()

    opposite.wait_recv()
    for h in range(2 * part):
        full = part_sums[base // near, h] + part_in[h].astype(jnp.float32)
        near_out[:, h] = full.astype(jnp.bfloat16).reshape(near, depth, width)
    back_copies = {
        d: mate_copy(near_out.at[mate_places[d]], back_in.at[place], back_send, back_recv, d)
        for d in range(1, near)
    }
    for copy in back_copies.values():
        copy.start()

    relays = []

    def pass_mid(block, group, source):
        block = block.astype(jnp.float32).reshape(2 * part, depth, width)
        mid[core, group, source] = swap_major(block).astype(jnp.bfloat16)
        n = len(relays)
        relays.append(
            pltpu.make_async_remote_copy(
                src_ref=mid.at[core, group, source],
                dst_ref=mid.at[core, group, source],
                send_sem=relay_send.at[n],
                recv_sem=relay_recv.at[n],
                device_id=partner,
                device_id_type=MESH,
            )
        )
        relays[n].start()

    pass_mid(near_out[place], 1, place)
    for d in range(1, near):
        back_copies[d].wait_recv()
        pass_mid(back_in[from_places[d]], 1, from_places[d])
    tri_in[me] = tri_out[me]
    for d in order:
        tri_copies[d].wait_recv()
    for d in range(near):
        source = from_places[d]
        pass_mid(tri_in[pl.ds(2 * source, 2)], 0, source)
    for copy in relays:
        copy.wait_recv()

    out_gain = gains[:, 1].reshape(2 * half, width)
    out_weights = weights[5]
    for start in range(0, depth, step):
        updates = []
        for x in range(start, start + step):
            values = mid[:, :, :, x].astype(jnp.float32).reshape(2 * hidden, width)
            operand = centred_unit(values, out_gain)
            projected = jnp.dot(out_weights, operand, preferred_element_type=jnp.float32)
            updates.append((gates[x] * projected)[None])
        stacked = swap_major(jnp.concatenate(updates, axis=0))
        out_ref[:, pl.ds(start, step)] = stacked.astype(jnp.bfloat16)

    for swap in swaps:
        swap.wait_send()
    opposite.wait_send()
    for copies in (*first_copies, near_copies, back_copies, tri_copies):
        for copy in copies.values():
            copy.wait_send()
    for copy in relays:
        copy.wait_send()


def fused_device(
    rows, pair_act, in_gain, left_proj, left_gate, right_proj, right_gate, out_gate, out_gain, out_proj
):
    half, depth, width = pair_act.shape
    hidden = left_proj.shape[1]
    part = hidden // rows // 2
    channels = 2 * half
    near = rows // 2
    anywhere = pl.BlockSpec(memory_space=pl.ANY)
    local = pl.BlockSpec(memory_space=pltpu.VMEM)
    bf16 = jnp.bfloat16
    dma = pltpu.SemaphoreType.DMA
    return pl.pallas_call(
        functools.partial(fused_kernel, rows),
        out_shape=pltpu.VMEM(pair_act.shape, bf16),
        in_specs=[anywhere, local] + [anywhere] * 5 + [local, anywhere],
        out_specs=local,
        scratch_shapes=[
            pltpu.VMEM((half, depth, width), bf16),
            pltpu.VMEM((2, depth, half, width), bf16),
            pltpu.VMEM((2, 2, half, width), jnp.float32),
            pltpu.VMEM((6, hidden, channels), bf16),
            pltpu.VMEM((2, 2 * hidden, channels), bf16),
            pltpu.VMEM((depth, channels, width), bf16),
            pltpu.VMEM((depth, hidden, width), jnp.float32),
            pltpu.VMEM((2, rows, depth, 2 * part, width), bf16),
            pltpu.VMEM((1, rows, depth, 2 * part, width), bf16),
            pltpu.VMEM((2 * part, rows * depth, width), bf16),
            pltpu.VMEM((rows, part, depth, width), bf16),
            pltpu.VMEM((rows, part, depth, width), bf16),
            pltpu.VMEM((2, 2, near, depth, 2 * part, width), bf16),
            pltpu.VMEM((near, 2, depth, 2 * part, width), bf16),
            pltpu.VMEM((2, 2 * part, near * depth, width), bf16),
            pltpu.VMEM((2, 2 * part, near * depth, width), jnp.float32),
            pltpu.VMEM((2 * part, near * depth, width), bf16),
            pltpu.VMEM((2 * part, near * depth, width), bf16),
            pltpu.VMEM((near, 2 * part, depth, width), bf16),
            pltpu.VMEM((near, 2 * part, depth, width), bf16),
            dma((7,)),
            dma((3,)),
            dma((3,)),
            dma((3, rows)),
            dma((3, rows)),
            dma((rows,)),
            dma((rows,)),
            dma((rows,)),
            dma((rows,)),
            dma((near,)),
            dma((near,)),
            dma((1,)),
            dma((1,)),
            dma((near,)),
            dma((near,)),
        ],
        compiler_params=pltpu.CompilerParams(collective_id=0, has_side_effects=True),
        name="triangle",
    )(
        pair_act,
        in_gain[None],
        left_proj.T,
        left_gate.T,
        right_proj.T,
        right_gate.T,
        out_gate.T,
        out_gain[None],
        out_proj.T,
    )


def dispatch(sizes, *args):
    half, depth, width = args[0].shape
    hidden = args[2].shape[1]
    rows = sizes["row"]
    fits = (
        sizes["col"] == 1
        and sizes["ch"] == 2
        and width == rows * depth
        and half == hidden
        and hidden % (8 * rows) == 0
        and depth % 16 == 0
        and rows % 2 == 0
        and width % 128 == 0
    )
    if fits:
        return fused_device(rows, *args)
    return per_device(*args)


def solution(mesh):
    return jax.shard_map(
        functools.partial(dispatch, dict(mesh.shape)),
        mesh=mesh,
        in_specs=(
            P("ch", ("grp", "row"), "col"),
            P("ch"),
            P(None, "ch"),
            P(None, "ch"),
            P(None, "ch"),
            P(None, "ch"),
            P(None, "ch"),
            P("ch"),
            P(None, "ch"),
        ),
        out_specs=P("ch", ("grp", "row"), "col"),
        check_vma=False,
    )
```

```python
import functools

import jax
import jax.numpy as jnp
from jax import lax
from jax.experimental import pallas as pl
from jax.experimental.pallas import tpu as pltpu
from jax.sharding import PartitionSpec as P


def spread_2(value, axis, source):
    kept = jnp.where(lax.axis_index(axis) == source, value, 0).astype(value.dtype)
    return lax.psum(kept, axis)


def moments(values, channel_count):
    first_sums, squares = lax.psum(
        (jnp.sum(values, axis=0), jnp.sum(values * values, axis=0)), "ch"
    )
    average = first_sums / channel_count
    spread = squares / channel_count - average * average
    centred = values - average[None]
    return centred * lax.rsqrt(spread + 1e-05)[None]


def per_device(
    pair_act, in_gain, left_proj, left_gate, right_proj, right_gate, out_gate, out_gain, out_proj
):
    row_count = pair_act.shape[1]
    col_count = pair_act.shape[2]
    hidden = left_proj.shape[1]
    fan_out = col_count // row_count
    normed = (
        moments(pair_act.astype(jnp.float32), pair_act.shape[0] * lax.axis_size("ch"))
        * in_gain[:, None, None]
    ).astype(jnp.bfloat16)
    whole = lax.all_gather(normed, "ch", axis=0, tiled=True)
    left_weights = jnp.concatenate((left_proj, left_gate), axis=1)
    left_lifted = jnp.einsum("cxy,cn->nyx", whole, left_weights, preferred_element_type=jnp.float32)
    left_edge = (jax.nn.sigmoid(left_lifted[hidden:]) * left_lifted[:hidden]).astype(jnp.bfloat16)
    other_weights = jnp.concatenate((right_proj, right_gate, out_gate), axis=1)
    other_lifted = jnp.einsum(
        "cxy,cn->nxy", whole, other_weights, preferred_element_type=jnp.float32
    )
    right_edge = (jax.nn.sigmoid(other_lifted[hidden : 2 * hidden]) * other_lifted[:hidden]).astype(
        jnp.bfloat16
    )
    gate_map = jax.nn.sigmoid(other_lifted[2 * hidden :])
    blocks = left_edge.reshape(hidden, fan_out, row_count, row_count)
    outgoing = jnp.tile(blocks, (1, lax.axis_size("row") // fan_out, 1, 1))
    arrived = lax.all_to_all(outgoing, "row", split_axis=1, concat_axis=3, tiled=True)
    left_panel = arrived.reshape(hidden, row_count, -1)
    left_panel = spread_2(left_panel, "col", lax.axis_index("row") // fan_out)
    tri_sum = jnp.einsum(
        "hik,hkj->hij",
        left_panel,
        lax.all_gather(right_edge, "row", axis=1, tiled=True),
        preferred_element_type=jnp.float32,
    )
    mid_norm = (moments(tri_sum, hidden * lax.axis_size("ch")) * out_gain[:, None, None]).astype(
        jnp.bfloat16
    )
    all_mid = lax.all_gather(mid_norm, "ch", axis=0, tiled=True)
    projected = jnp.einsum("hxy,hc->cxy", all_mid, out_proj, preferred_element_type=jnp.float32)
    return (gate_map * projected).astype(jnp.bfloat16)


MESH = pl.DeviceIdType.MESH


def swap_major(values):
    return jnp.swapaxes(values, 0, 1)


def spread_gain(gain, lanes):
    return jnp.broadcast_to(gain, (lanes, gain.shape[1])).T


def centred_unit(values, gain):
    count = values.shape[0]
    average = jnp.sum(values, axis=0, keepdims=True) / count
    centred = values - average
    spread = jnp.sum(centred * centred, axis=0, keepdims=True) / count
    return (centred * lax.rsqrt(spread + 1e-05) * gain).astype(jnp.bfloat16)


def fused_kernel(
    rows,
    act_ref,
    gain_ref,
    lp_ref,
    lg_ref,
    rp_ref,
    rg_ref,
    og_ref,
    gain2_ref,
    op_ref,
    out_ref,
    raw,
    act,
    gains,
    weights,
    edge_weights,
    normed,
    gates,
    outbox,
    inbox,
    edges,
    tri_out,
    tri_in,
    mid,
    near_in,
    near_edges,
    part_sums,
    part_out,
    part_in,
    near_out,
    back_in,
    load_sem,
    pair_send,
    pair_recv,
    lr_send,
    lr_recv,
    tri_send,
    tri_recv,
    relay_send,
    relay_recv,
    near_send,
    near_recv,
    part_send,
    part_recv,
    back_send,
    back_recv,
):
    me = lax.axis_index("row")
    core = lax.axis_index("ch")
    other = 1 - core
    half, depth, width = act_ref.shape
    hidden = lp_ref.shape[0]
    part = hidden // rows // 2
    partner = {"ch": other}
    peers = [lax.rem(me + d, rows) for d in range(rows)]
    sources = [lax.rem(me + rows - d, rows) for d in range(rows)]
    order = sorted(range(1, rows), key=lambda d: -min(d, rows - d))
    step = depth // 2
    near = rows // 2
    base = me // near * near
    place = me - base
    far_base = near - base
    mates = [base + lax.rem(place + d, near) for d in range(near)]
    mate_places = [lax.rem(place + d, near) for d in range(near)]
    from_places = [lax.rem(place + near - d, near) for d in range(near)]
    halves = (pl.ds(0, step), pl.ds(step, step))

    loads = [pltpu.make_async_copy(act_ref, raw, load_sem.at[0])]
    for n, ref in enumerate((lp_ref, lg_ref, rp_ref, rg_ref, og_ref, op_ref)):
        loads.append(pltpu.make_async_copy(ref, weights.at[n], load_sem.at[n + 1]))
    for load in loads:
        load.start()
    barrier = pltpu.get_barrier_semaphore()
    pl.semaphore_signal(barrier, inc=1, device_id=partner, device_id_type=MESH)
    for d in range(1, rows):
        pl.semaphore_signal(barrier, inc=1, device_id={"row": peers[d]}, device_id_type=MESH)
    gains[core, 0] = spread_gain(gain_ref[...], width)
    gains[core, 1] = spread_gain(gain2_ref[...], width)
    loads[0].wait()
    for n in range(2):
        turned = swap_major(raw[:, halves[n]].astype(jnp.float32))
        act[core, halves[n]] = turned.astype(jnp.bfloat16)

    def to_partner(ref, n):
        return pltpu.make_async_remote_copy(
            src_ref=ref,
            dst_ref=ref,
            send_sem=pair_send.at[n],
            recv_sem=pair_recv.at[n],
            device_id=partner,
            device_id_type=MESH,
        )

    pl.semaphore_wait(barrier, rows)
    swaps = [
        to_partner(gains.at[core], 2),
        to_partner(act.at[core, halves[0]], 0),
        to_partner(act.at[core, halves[1]], 1),
    ]
    for swap in swaps:
        swap.start()
    for load in loads[1:]:
        load.wait()
    for n in range(2):
        first = weights[n].astype(jnp.float32).reshape(2, rows, part, 2 * half)
        second = weights[n + 2].astype(jnp.float32).reshape(2, rows, part, 2 * half)
        joined = jnp.concatenate((first, second), axis=2)
        edge_weights[n] = joined.reshape(2 * hidden, 2 * half).astype(jnp.bfloat16)

    def edge_copy(n, src, dst, d):
        return pltpu.make_async_remote_copy(
            src_ref=src,
            dst_ref=dst,
            send_sem=lr_send.at[n, d],
            recv_sem=lr_recv.at[n, d],
            device_id={"row": peers[d]},
            device_id_type=MESH,
        )

    first_copies = [
        {
            d: edge_copy(n, outbox.at[0, peers[d]], inbox.at[0, me], d)
            for d in order
        }
        for n in range(1)
    ]

    def mate_copy(src, dst, sends, recvs, d):
        return pltpu.make_async_remote_copy(
            src_ref=src,
            dst_ref=dst,
            send_sem=sends.at[d],
            recv_sem=recvs.at[d],
            device_id={"row": mates[d]},
            device_id_type=MESH,
        )

    near_copies = {
        d: mate_copy(
            outbox.at[1, pl.ds(2 * mate_places[d], 2)],
            near_in.at[place],
            near_send,
            near_recv,
            d,
        )
        for d in range(1, near)
    }

    swaps[0].wait_recv()
    in_gain = gains[:, 0].reshape(2 * half, width)
    lift_weights = edge_weights[...].reshape(4 * hidden, 2 * half)
    for n in range(2):
        swaps[1 + n].wait_recv()
        for x in range(n * step, (n + 1) * step):
            values = act[:, x].astype(jnp.float32).reshape(2 * half, width)
            operand = centred_unit(values, in_gain)
            normed[x] = operand
            lifted = jnp.dot(lift_weights, operand, preferred_element_type=jnp.float32)
            both = jax.nn.sigmoid(lifted[2 * hidden :]) * lifted[: 2 * hidden]
            both = both.reshape(2, rows, 2 * part, width).astype(jnp.bfloat16)
            outbox[0, :, x] = both[0]
            outbox[1, :, x] = both[1]

    for copy in near_copies.values():
        copy.start()
    for d in order:
        first_copies[0][d].start()

    def take_edges(box, source):
        turned = swap_major(box.astype(jnp.float32)).astype(jnp.bfloat16)
        edges[:, pl.ds(pl.multiple_of(source * depth, depth), depth)] = turned

    def take_near(boxes, source):
        for n in range(2):
            turned = swap_major(boxes[n].astype(jnp.float32)).astype(jnp.bfloat16)
            near_edges[n, :, pl.ds(pl.multiple_of(source * depth, depth), depth)] = turned

    take_edges(outbox[0, me], me)
    take_near(outbox.at[1, pl.ds(2 * place, 2)], place)
    gate_weights = weights[4]
    for x in range(depth):
        gates[x] = jax.nn.sigmoid(
            jnp.dot(gate_weights, normed[x], preferred_element_type=jnp.float32)
        )

    def contract(first, second):
        return lax.dot_general(
            first, second, (((0,), (0,)), ((), ())), preferred_element_type=jnp.float32
        )

    for d in range(1, near):
        near_copies[d].wait_recv()
        take_near(near_in.at[from_places[d]], from_places[d])
    for n in range(2):
        for h in range(part):
            partial = contract(near_edges[n, h], near_edges[n, part + h])
            part_sums[:, n * part + h] = partial.reshape(2, near * depth, width)
    part_out[...] = part_sums[far_base // near].astype(jnp.bfloat16)
    opposite = pltpu.make_async_remote_copy(
        src_ref=part_out,
        dst_ref=part_in,
        send_sem=part_send.at[0],
        recv_sem=part_recv.at[0],
        device_id={"row": far_base + place},
        device_id_type=MESH,
    )
    opposite.start()

    tri_copies = {
        d: pltpu.make_async_remote_copy(
            src_ref=tri_out.at[peers[d]],
            dst_ref=tri_in.at[me],
            send_sem=tri_send.at[d],
            recv_sem=tri_recv.at[d],
            device_id={"row": peers[d]},
            device_id_type=MESH,
        )
        for d in order
    }
    for d in order:
        first_copies[0][d].wait_recv()
        take_edges(inbox[0, sources[d]], sources[d])
    for h in range(part):
        tri_sum = contract(edges[h], edges[part + h])
        tri_out[:, h] = tri_sum.astype(jnp.bfloat16).reshape(rows, depth, width)
    for d in order:
        tri_copies[d].start()

    opposite.wait_recv()
    for h in range(2 * part):
        full = part_sums[base // near, h] + part_in[h].astype(jnp.float32)
        near_out[:, h] = full.astype(jnp.bfloat16).reshape(near, depth, width)
    back_copies = {
        d: mate_copy(near_out.at[mate_places[d]], back_in.at[place], back_send, back_recv, d)
        for d in range(1, near)
    }
    for copy in back_copies.values():
        copy.start()

    relays = []

    def pass_mid(block, group, source):
        block = block.astype(jnp.float32).reshape(2 * part, depth, width)
        mid[core, group, source] = swap_major(block).astype(jnp.bfloat16)
        n = len(relays)
        relays.append(
            pltpu.make_async_remote_copy(
                src_ref=mid.at[core, group, source],
                dst_ref=mid.at[core, group, source],
                send_sem=relay_send.at[n],
                recv_sem=relay_recv.at[n],
                device_id=partner,
                device_id_type=MESH,
            )
        )
        relays[n].start()

    pass_mid(near_out[place], 1, place)
    for d in range(1, near):
        back_copies[d].wait_recv()
        pass_mid(back_in[from_places[d]], 1, from_places[d])
    tri_in[me] = tri_out[me]
    for d in order:
        tri_copies[d].wait_recv()
    for d in range(near):
        source = from_places[d]
        pass_mid(tri_in[pl.ds(2 * source, 2)], 0, source)
    for copy in relays:
        copy.wait_recv()

    out_gain = gains[:, 1].reshape(2 * half, width)
    out_weights = weights[5]
    for start in range(0, depth, step):
        updates = []
        for x in range(start, start + step):
            values = mid[:, :, :, x].astype(jnp.float32).reshape(2 * hidden, width)
            operand = centred_unit(values, out_gain)
            projected = jnp.dot(out_weights, operand, preferred_element_type=jnp.float32)
            updates.append((gates[x] * projected)[None])
        stacked = swap_major(jnp.concatenate(updates, axis=0))
        out_ref[:, pl.ds(start, step)] = stacked.astype(jnp.bfloat16)

    for swap in swaps:
        swap.wait_send()
    opposite.wait_send()
    for copies in (*first_copies, near_copies, back_copies, tri_copies):
        for copy in copies.values():
            copy.wait_send()
    for copy in relays:
        copy.wait_send()


def fused_device(
    rows, pair_act, in_gain, left_proj, left_gate, right_proj, right_gate, out_gate, out_gain, out_proj
):
    half, depth, width = pair_act.shape
    hidden = left_proj.shape[1]
    part = hidden // rows // 2
    channels = 2 * half
    near = rows // 2
    anywhere = pl.BlockSpec(memory_space=pl.ANY)
    local = pl.BlockSpec(memory_space=pltpu.VMEM)
    bf16 = jnp.bfloat16
    dma = pltpu.SemaphoreType.DMA
    return pl.pallas_call(
        functools.partial(fused_kernel, rows),
        out_shape=pltpu.VMEM(pair_act.shape, bf16),
        in_specs=[anywhere, local] + [anywhere] * 5 + [local, anywhere],
        out_specs=local,
        scratch_shapes=[
            pltpu.VMEM((half, depth, width), bf16),
            pltpu.VMEM((2, depth, half, width), bf16),
            pltpu.VMEM((2, 2, half, width), jnp.float32),
            pltpu.VMEM((6, hidden, channels), bf16),
            pltpu.VMEM((2, 2 * hidden, channels), bf16),
            pltpu.VMEM((depth, channels, width), bf16),
            pltpu.VMEM((depth, hidden, width), jnp.float32),
            pltpu.VMEM((2, rows, depth, 2 * part, width), bf16),
            pltpu.VMEM((1, rows, depth, 2 * part, width), bf16),
            pltpu.VMEM((2 * part, rows * depth, width), bf16),
            pltpu.VMEM((rows, part, depth, width), bf16),
            pltpu.VMEM((rows, part, depth, width), bf16),
            pltpu.VMEM((2, 2, near, depth, 2 * part, width), bf16),
            pltpu.VMEM((near, 2, depth, 2 * part, width), bf16),
            pltpu.VMEM((2, 2 * part, near * depth, width), bf16),
            pltpu.VMEM((2, 2 * part, near * depth, width), jnp.float32),
            pltpu.VMEM((2 * part, near * depth, width), bf16),
            pltpu.VMEM((2 * part, near * depth, width), bf16),
            pltpu.VMEM((near, 2 * part, depth, width), bf16),
            pltpu.VMEM((near, 2 * part, depth, width), bf16),
            dma((7,)),
            dma((3,)),
            dma((3,)),
            dma((3, rows)),
            dma((3, rows)),
            dma((rows,)),
            dma((rows,)),
            dma((rows,)),
            dma((rows,)),
            dma((near,)),
            dma((near,)),
            dma((1,)),
            dma((1,)),
            dma((near,)),
            dma((near,)),
        ],
        compiler_params=pltpu.CompilerParams(collective_id=0, has_side_effects=True),
        name="triangle",
    )(
        pair_act,
        in_gain[None],
        left_proj.T,
        left_gate.T,
        right_proj.T,
        right_gate.T,
        out_gate.T,
        out_gain[None],
        out_proj.T,
    )


def dispatch(sizes, *args):
    half, depth, width = args[0].shape
    hidden = args[2].shape[1]
    rows = sizes["row"]
    fits = (
        sizes["col"] == 1
        and sizes["ch"] == 2
        and width == rows * depth
        and half == hidden
        and hidden % (8 * rows) == 0
        and depth % 16 == 0
        and rows % 2 == 0
        and width % 128 == 0
    )
    if fits:
        return fused_device(rows, *args)
    return per_device(*args)


def solution(mesh):
    return jax.shard_map(
        functools.partial(dispatch, dict(mesh.shape)),
        mesh=mesh,
        in_specs=(
            P("ch", ("grp", "row"), "col"),
            P("ch"),
            P(None, "ch"),
            P(None, "ch"),
            P(None, "ch"),
            P(None, "ch"),
            P(None, "ch"),
            P("ch"),
            P(None, "ch"),
        ),
        out_specs=P("ch", ("grp", "row"), "col"),
        check_vma=False,
    )
```
